128 devices in a mesh: gx: 16 (over x, z), gy: 8 (over y, core).
Axes of the slice: x: 4, y: 4, z: 4, core: 2. Of those that a mesh axis runs over, the one named last changes fastest.
Arguments:
- velocity: float32 [3, 256, 512, 256], P(None, 'gx', 'gy'), may hold values from -6 to 6
Outputs:
- details_one: float32 [7, 9, 128, 256, 128], P(None, None, 'gx', 'gy')
- stress_one: float32 [6, 128, 256, 128], P(None, 'gx', 'gy')
- details_two: float32 [7, 9, 64, 128, 64], P(None, None, 'gx', 'gy')
- stress_two: float32 [6, 64, 128, 64], P(None, 'gx', 'gy')
- details_three: float32 [7, 9, 32, 64, 32], P(None, None, 'gx', 'gy')
- stress_three: float32 [6, 32, 64, 32], P(None, 'gx', 'gy')
- coarse_velocity: float32 [3, 32, 64, 32], P(None, 'gx', 'gy')
The draws below stay inside these ranges and needn't reach their ends.
All inputs are finite; a program needn't handle non-finite values.
Results may differ from the reference program's by a relative error of at most 0.0003.
Values sent between devices are 32-bit elements; how exact they have to be, the bound alone decides.
A program may use at most 256 MiB of HBM per device.

```python
import jax
import jax.numpy as jnp
from jax import lax

NZ = 256
NX = 256
NY = 512


def block_scale(own_key, shape, shards, low, high):
    def one(axis_at, parts):
        steps = jax.random.uniform(jax.random.fold_in(jax.random.fold_in(own_key, 6), axis_at), (parts,), jnp.float32, low / len(shards), high / len(shards))
        return jnp.repeat(jnp.exp(steps), shape[axis_at] // parts).reshape((-1,) + (1,) * (len(shape) - axis_at - 1))

    level = one(*shards[0])
    for cut in shards[1:]:
        level = level * one(*cut)
    return level


def gaussian(rng, shape, scale, limit, shards=(), dtype=jnp.bfloat16):
    factor_of = block_scale(rng, shape, shards, -0.22, 0.18) if shards else 1.0
    result = jax.random.normal(rng, shape, jnp.float32) * scale * factor_of
    return jnp.minimum(jnp.maximum(result, -limit), limit).astype(dtype)


def setup_inputs(seed: int = 0) -> dict:
    keys = jax.random.split(jax.random.key(seed), 2)
    velocity = gaussian(keys[0], (3, NX, NY, NZ), 1.0, 6.0, ((1, 16), (2, 8)), jnp.float32)
    return {"velocity": velocity}


predict_one = -1.586134342
update_one = -0.05298011854
predict_two = 0.8829110762
update_two = 0.4435068522
scaling = 1.149604398
product_pairs = ((0, 0), (0, 1), (0, 2), (1, 1), (1, 2), (2, 2))


def lifting(volume, dimension, next_even, prev_odd):
    length = volume.shape[dimension]
    even_cells = lax.slice_in_dim(volume, 0, length, 2, dimension)
    odd_cells = lax.slice_in_dim(volume, 1, length, 2, dimension)
    odd_cells = odd_cells + predict_one * (even_cells + next_even(even_cells))
    even_cells = even_cells + update_one * (odd_cells + prev_odd(odd_cells))
    odd_cells = odd_cells + predict_two * (even_cells + next_even(even_cells))
    even_cells = even_cells + update_two * (odd_cells + prev_odd(odd_cells))
    return jnp.concatenate([even_cells * scaling, odd_cells / scaling], axis=0)


def periodic_next(dimension):
    return lambda values: jnp.roll(values, -1, axis=dimension)


def periodic_prev(dimension):
    return lambda values: jnp.roll(values, 1, axis=dimension)


def mirror_next(dimension):
    def shifted(values):
        extent = values.shape[dimension]
        return jnp.concatenate([lax.slice_in_dim(values, 1, extent, 1, dimension), lax.slice_in_dim(values, extent - 1, extent, 1, dimension)], axis=dimension)
    return shifted


def mirror_prev(dimension):
    def shifted(values):
        extent = values.shape[dimension]
        return jnp.concatenate([lax.slice_in_dim(values, 0, 1, 1, dimension), lax.slice_in_dim(values, 0, extent - 1, 1, dimension)], axis=dimension)
    return shifted


def stresses_of(approximation):
    return jnp.stack([approximation[3 + position] - approximation[pair[0]] * approximation[pair[1]] for position, pair in enumerate(product_pairs)])


def reference(velocity):
    products = jnp.stack([velocity[pair[0]] * velocity[pair[1]] for pair in product_pairs])
    all_fields = jnp.concatenate([velocity, products], axis=0)
    results = []
    for level_index in range(3):
        subbands = lifting(all_fields, 1, periodic_next(1), periodic_prev(1))
        subbands = lifting(subbands, 2, periodic_next(2), periodic_prev(2))
        subbands = lifting(subbands, 3, mirror_next(3), mirror_prev(3))
        grouped = subbands.reshape((8, 9) + subbands.shape[1:])
        approximation = grouped[0]
        results.append(grouped[1:])
        results.append(stresses_of(approximation))
        all_fields = approximation
    return (results[0], results[1], results[2], results[3], results[4], results[5], approximation[:3])
```

```python
import jax
import jax.numpy as jnp
import numpy as np
from jax import lax
from jax.experimental import pallas as pl
from jax.experimental.pallas import tpu as pltpu
from jax.sharding import PartitionSpec as P

MESH = pl.DeviceIdType.MESH
F32 = jnp.float32
BF16 = jnp.bfloat16

predict_one = -1.586134342
update_one = -0.05298011854
predict_two = 0.8829110762
update_two = 0.4435068522
scaling = 1.149604398
product_pairs = ((0, 0), (0, 1), (0, 2), (1, 1), (1, 2), (2, 2))


def third_table(length, rows):
    identity = np.eye(length)
    even, odd = identity[:, 0::2], identity[:, 1::2]

    def ahead(values):
        return np.concatenate([values[:, 1:], values[:, -1:]], axis=1)

    def behind(values):
        return np.concatenate([values[:, :1], values[:, :-1]], axis=1)

    odd = odd + predict_one * (even + ahead(even))
    even = even + update_one * (odd + behind(odd))
    odd = odd + predict_two * (even + ahead(even))
    even = even + update_two * (odd + behind(odd))
    table = np.zeros((rows, 256))
    table[:length, : length // 2] = even * scaling
    table[:length, 128 : 128 + length // 2] = odd / scaling
    one = table.astype(np.float32).astype(BF16)
    two = (table - one.astype(np.float64)).astype(np.float32).astype(BF16)
    three = (table - one.astype(np.float64) - two.astype(np.float64)).astype(np.float32).astype(BF16)
    return np.concatenate([one, two, one, two, three, one], axis=0)


class Lift:
    def __init__(self, cell):
        self.cell = cell
        self.known = {}

    def get(self, key, make):
        if key not in self.known:
            self.known[key] = make()
        return self.known[key]

    def even(self, i):
        return self.get(("e", i), lambda: self.cell(2 * i))

    def odd(self, i):
        return self.get(("o", i), lambda: self.cell(2 * i + 1))

    def odd_one(self, i):
        return self.get(("o1", i), lambda: self.odd(i) + predict_one * (self.even(i) + self.even(i + 1)))

    def even_one(self, i):
        return self.get(("e1", i), lambda: self.even(i) + update_one * (self.odd_one(i - 1) + self.odd_one(i)))

    def high(self, i):
        return self.get(("o2", i), lambda: self.odd_one(i) + predict_two * (self.even_one(i) + self.even_one(i + 1)))

    def low(self, i):
        return self.get(("e2", i), lambda: self.even_one(i) + update_two * (self.high(i - 1) + self.high(i)))


def loop(count, body):
    def step(i, carry):
        body(i)
        return carry

    lax.fori_loop(0, count, step, 0)


def split_store(target, row, lane, value):
    one = value.astype(BF16)
    rest = value - one.astype(F32)
    two = rest.astype(BF16)
    three = (rest - two.astype(F32)).astype(BF16)
    rows = pl.ds(row, 16)
    target[0, rows, lane : lane + 128] = one
    target[1, rows, lane : lane + 128] = two
    target[2, rows, lane : lane + 128] = three


def along_y(load, block, x_high, store):
    lift = Lift(load)
    half = block // 2
    values = []
    for i in range(half):
        value = lift.low(i)
        values.append(value if x_high else value * (scaling * scaling))
    for i in range(half):
        value = lift.high(i)
        values.append(value * (1.0 / (scaling * scaling)) if x_high else value)
    for n in range(0, block, 2):
        store(n * 8, jnp.concatenate([values[n], values[n + 1]], axis=0))


def along_z(split, table, row, rows):
    at = pl.ds(row, rows)
    one, two, three = split[0, at, :], split[1, at, :], split[2, at, :]
    left = jnp.concatenate([one, one, two, two, one, three], axis=1)
    return jnp.dot(left, table[...], preferred_element_type=F32)


def kernel(count_x, count_y, v, t1, t2, t3, d1, s1, d2, s2, d3, s3, coarse,
           cells, bands, split, second, third, last, stage, w1, w2, w3,
           cs1, cr1, cs2, cr2, cs3, cr3, bands_low, split_low, own_sem, send_sem, recv_sem):
    gx, gy = lax.axis_index("gx"), lax.axis_index("gy")
    right, left = lax.rem(gx + 1, count_x), lax.rem(gx + count_x - 1, count_x)
    up, down = lax.rem(gy + 1, count_y), lax.rem(gy + count_y - 1, count_y)
    corners = ((right, up), (right, down), (left, up), (left, down))
    around = ((right, gy), (left, gy), (gx, up), (gx, down)) + corners

    own = [pltpu.make_async_copy(v.at[c], cells.at[c, 4:20, 8:72, :], own_sem.at[c]) for c in range(3)]
    tables = [pltpu.make_async_copy(src, dst, own_sem.at[3 + n]) for n, (src, dst) in enumerate(((t1, w1), (t2, w2), (t3, w3)))]
    for copy in own:
        copy.start()
    barrier = pltpu.get_barrier_semaphore()
    for device in around:
        pl.semaphore_signal(barrier, inc=1, device_id=device, device_id_type=MESH)
    for copy in tables:
        copy.start()
    pl.semaphore_wait(barrier, 8)

    started = []

    def send(src, dst, device):
        n = len(started)
        copy = pltpu.make_async_remote_copy(
            src_ref=src, dst_ref=dst, send_sem=send_sem.at[n], recv_sem=recv_sem.at[n], device_id=device, device_id_type=MESH
        )
        copy.start()
        started.append(copy)
        return copy

    def send_x(c):
        return (
            send(v.at[c, 12:16], cells.at[c, 0:4, 8:72, :], (right, gy)),
            send(v.at[c, 0:3], cells.at[c, 20:23, 8:72, :], (left, gy)),
        )

    x_halo = [send_x(0)]
    y_halo = (
        send(v.at[:, :, 56:64, :], cells.at[0:3, 4:20, 0:8, :], (gx, up)),
        send(v.at[:, :, 0:8, :], cells.at[0:3, 4:20, 72:80, :], (gx, down)),
    )
    for copy in own:
        copy.wait()
    for k, (layer, row) in enumerate(((16, 68), (16, 8), (4, 68), (4, 8))):
        for c in range(3):
            for m in range(2):
                for u in range(2):
                    cs1[k, c, m, 4 * u : 4 * u + 4, :] = cells[c, layer + 2 * m + u, row : row + 4, :]

    def fill(i):
        cells[3, i] = jnp.ones((80, 256), F32)

    loop(23, fill)
    corner_halo = [send(cs1.at[k], cr1.at[k], corners[k]) for k in range(4)]
    x_halo += [send_x(1), send_x(2)]
    for copy in tables:
        copy.wait()
    for copy in y_halo:
        copy.wait_recv()

    def level_one(g, lows, highs):
        wanted = [(0, k) for k in lows] + [(1, k) for k in highs]

        def field(t):
            other = lax.rem(t + 3, 4)
            index = 3 + lax.div((t + 1) * (6 - t), 2) + g - (6 - t)

            def along_x(i):
                rows = pl.ds(pl.multiple_of(i * 8, 8), 8)
                for h in range(2):
                    lanes = slice(128 * h, 128 * h + 128)
                    lift = Lift(lambda n: cells[g, 4 + n, rows, lanes] * cells[other, 4 + n, rows, lanes])
                    for n, (x_high, k) in enumerate(wanted):
                        bands[n, h, rows, :] = lift.high(k) if x_high else lift.low(k)

            loop(10, along_x)

            def y_band(x_high):
                def one(n):
                    n = n + len(lows) if x_high else n
                    for h in range(2):
                        along_y(
                            lambda r: bands[n, h, pl.ds(8 + r, 8, stride=8), :],
                            8,
                            x_high,
                            lambda at, value: split_store(split, pl.multiple_of(n * 64 + at, 16), 128 * h, value),
                        )

                return one

            loop(len(lows), y_band(0))
            loop(len(highs), y_band(1))
            for n, (x_high, k) in enumerate(wanted):
                out = along_z(split, w1, n * 64, 64)
                for y_high in range(2):
                    for j in range(4):
                        at = y_high * 32 + j * 8
                        for z_high in range(2):
                            value = out[at : at + 8, 128 * z_high : 128 * z_high + 128]
                            band = 4 * z_high + 2 * y_high + x_high
                            if band:
                                d1[band - 1, index, k, pl.ds(j, 8, stride=4), :] = value
                            else:
                                second[index, k, pl.ds(8 + j, 8, stride=4), :] = value

        loop(g + 2, field)

    for g in range(3):
        level_one(g, (2, 3, 4, 5), (1, 2, 3, 4, 5))
    for g in range(3):
        for copy in x_halo[g]:
            copy.wait_recv()
        if g == 0:
            for copy in corner_halo:
                copy.wait_recv()
            for k, (layer, row) in enumerate(((0, 4), (0, 72), (20, 4), (20, 72))):
                for c in range(3):
                    for m in range(2):
                        for u in range(2):
                            if layer + 2 * m + u < 23:
                                cells[c, layer + 2 * m + u, row : row + 4, :] = cr1[k, c, m, 4 * u : 4 * u + 4, :]
        level_one(g, (0, 1, 6, 7), (0, 6, 7))

    def exchange(field, n, rows, cs, cr):
        def prepare(f):
            def tile(i):
                at = pl.ds(pl.multiple_of(8 + i * 8, 8), 8)
                layer = lambda l: field[f, l, at, :]
                field[f, n + 4, at, :] = layer(n - 1) + predict_one * layer(n - 2)
                before = layer(n - 3) + predict_one * (layer(n - 4) + layer(n - 2))
                field[f, n + 5, at, :] = layer(n - 2) + update_one * before
                field[f, n + 6, at, :] = layer(0)
                field[f, n + 7, at, :] = layer(1) + predict_one * (layer(0) + layer(2))

            for i in range(rows // 8):
                tile(i)
            for k, (layer, row) in enumerate(((n + 4, 4 + rows), (n + 4, 8), (n + 6, 4 + rows), (n + 6, 8))):
                for u in range(2):
                    cs[k, f, 4 * u : 4 * u + 4, :] = field[f, layer + u, row : row + 4, :]

        loop(9, prepare)
        whole = slice(8, 8 + rows)
        halo = [
            send(field.at[:, n + 4 : n + 6, whole, :], field.at[:, n : n + 2, whole, :], (right, gy)),
            send(field.at[:, n + 6 : n + 8, whole, :], field.at[:, n + 2 : n + 4, whole, :], (left, gy)),
        ]
        halo += [send(cs.at[k], cr.at[k], corners[k]) for k in range(4)]
        halo += [
            send(field.at[:, 0:n, rows : rows + 8, :], field.at[:, 0:n, 0:8, :], (gx, up)),
            send(field.at[:, 0:n, 8:16, :], field.at[:, 0:n, 8 + rows : 16 + rows, :], (gx, down)),
        ]

        def finish():
            for copy in halo:
                copy.wait_recv()

            def unpack(f):
                for k, (layer, row) in enumerate(((n, 4), (n, 8 + rows), (n + 2, 4), (n + 2, 8 + rows))):
                    for u in range(2):
                        field[f, layer + u, row : row + 4, :] = cr[k, f, 4 * u : 4 * u + 4, :]

            loop(9, unpack)

        return finish

    def stresses(target, field, n, at):
        def layer(l):
            for k, (p, q) in enumerate(product_pairs):
                value = field[3 + k, l, at, :] - field[p, l, at, :] * field[q, l, at, :]
                target[k, l] = value[:, : target.shape[3]]

        loop(n, layer)

    def level(field, n, rows, table, put):
        half = n // 2
        block = rows // 8

        def one_field(f):
            def along_x(i):
                at = pl.ds(pl.multiple_of(i * 8, 8), 8)
                lift = Lift(lambda l: field[f, l if l < n else n + 2, at, :])
                lift.known[("o1", -1)] = field[f, n, at, :] + predict_one * lift.even(0)
                lift.known[("e1", -1)] = field[f, n + 1, at, :] + update_one * lift.odd_one(-1)
                lift.known[("o1", half)] = field[f, n + 3, at, :]
                lift.known[("o2", -1)] = lift.odd_one(-1) + predict_two * (lift.even_one(-1) + lift.even_one(0))
                for k in range(half):
                    bands_low[k, at, :] = lift.low(k)
                    bands_low[half + k, at, :] = lift.high(k)

            loop(rows // 8 + 2, along_x)

            def y_band(x_high):
                def one(k):
                    k = k + half if x_high else k
                    along_y(
                        lambda r: bands_low[k, pl.ds(8 + r, 8, stride=block), :],
                        block,
                        x_high,
                        lambda at, value: split_store(split_low, pl.multiple_of(k * rows + at, 16), 0, value),
                    )

                return one

            loop(half, y_band(0))
            loop(half, y_band(1))
            out = along_z(split_low, table, 0, n * rows)
            for k in range(n):
                x_high, x_at = divmod(k, half)
                for y_high in range(2):
                    for j in range(block // 2):
                        at = k * rows + y_high * (rows // 2) + j * 8
                        for z_high in range(2):
                            value = out[at : at + 8, 128 * z_high : 128 * z_high + 128]
                            put(f, 4 * z_high + 2 * y_high + x_high, x_at, j, value)

        loop(9, one_field)

    finish = exchange(second, 8, 32, cs2, cr2)
    stresses(s1, second, 8, slice(8, 40))
    finish()

    def put_two(f, band, k, j, value):
        if band:
            stage[band - 1, k, pl.ds(j, 8, stride=2), :] = value
            if j == 1:
                d2[band - 1, f, k] = stage[band - 1, k][:, :64]
        else:
            third[f, k, pl.ds(8 + j, 8, stride=2), :] = value

    level(second, 8, 32, w2, put_two)
    finish = exchange(third, 4, 16, cs3, cr3)
    stresses(s2, third, 4, slice(8, 24))
    finish()

    def put_three(f, band, k, j, value):
        if band:
            d3[band - 1, f, k] = value[:, :32]
        else:
            last[f, k] = value

    level(third, 4, 16, w3, put_three)
    stresses(s3, last, 2, slice(0, 8))
    for c in range(3):
        coarse[c] = last[c][:, :, :32]
    for copy in started:
        copy.wait_send()


def body(velocity):
    shapes = ((7, 9, 8, 32, 128), (6, 8, 32, 128), (7, 9, 4, 16, 64), (6, 4, 16, 64), (7, 9, 2, 8, 32), (6, 2, 8, 32), (3, 2, 8, 32))
    copies = 12 + 8 + 8
    run = pl.pallas_call(
        lambda *refs: kernel(lax.axis_size("gx"), lax.axis_size("gy"), *refs),
        out_shape=[jax.ShapeDtypeStruct(shape, F32) for shape in shapes],
        in_specs=[pl.BlockSpec(memory_space=pltpu.HBM)] * 4,
        out_specs=[pl.BlockSpec(memory_space=pltpu.VMEM)] * 7,
        scratch_shapes=[
            pltpu.VMEM((4, 23, 80, 256), F32),
            pltpu.VMEM((9, 2, 80, 128), F32),
            pltpu.VMEM((3, 576, 256), BF16),
            pltpu.VMEM((9, 16, 48, 128), F32),
            pltpu.VMEM((9, 12, 32, 128), F32),
            pltpu.VMEM((9, 2, 8, 128), F32),
            pltpu.VMEM((7, 4, 16, 128), F32),
            pltpu.VMEM((1536, 256), BF16),
            pltpu.VMEM((768, 256), BF16),
            pltpu.VMEM((768, 256), BF16),
            pltpu.VMEM((4, 3, 2, 8, 256), F32),
            pltpu.VMEM((4, 3, 2, 8, 256), F32),
            pltpu.VMEM((4, 9, 8, 128), F32),
            pltpu.VMEM((4, 9, 8, 128), F32),
            pltpu.VMEM((4, 9, 8, 128), F32),
            pltpu.VMEM((4, 9, 8, 128), F32),
            pltpu.VMEM((8, 48, 128), F32),
            pltpu.VMEM((3, 256, 128), BF16),
            pltpu.SemaphoreType.DMA((6,)),
            pltpu.SemaphoreType.DMA((copies,)),
            pltpu.SemaphoreType.DMA((copies,)),
        ],
        compiler_params=pltpu.CompilerParams(collective_id=0, has_side_effects=True, vmem_limit_bytes=34 << 20),
    )
    return tuple(run(velocity, third_table(256, 256), third_table(128, 128), third_table(64, 128)))


def solution(mesh):
    in_specs = (P(None, "gx", "gy", None),)
    out_specs = (
        P(None, None, "gx", "gy", None),
        P(None, "gx", "gy", None),
        P(None, None, "gx", "gy", None),
        P(None, "gx", "gy", None),
        P(None, None, "gx", "gy", None),
        P(None, "gx", "gy", None),
        P(None, "gx", "gy", None),
    )
    return jax.shard_map(body, mesh=mesh, in_specs=in_specs, out_specs=out_specs, check_vma=False)
```

```python
import jax
import jax.numpy as jnp
import numpy as np
from jax import lax
from jax.experimental import pallas as pl
from jax.experimental.pallas import tpu as pltpu
from jax.sharding import PartitionSpec as P

MESH = pl.DeviceIdType.MESH
F32 = jnp.float32
BF16 = jnp.bfloat16

predict_one = -1.586134342
update_one = -0.05298011854
predict_two = 0.8829110762
update_two = 0.4435068522
scaling = 1.149604398
product_pairs = ((0, 0), (0, 1), (0, 2), (1, 1), (1, 2), (2, 2))


def third_table(length, rows):
    identity = np.eye(length)
    even, odd = identity[:, 0::2], identity[:, 1::2]

    def ahead(values):
        return np.concatenate([values[:, 1:], values[:, -1:]], axis=1)

    def behind(values):
        return np.concatenate([values[:, :1], values[:, :-1]], axis=1)

    odd = odd + predict_one * (even + ahead(even))
    even = even + update_one * (odd + behind(odd))
    odd = odd + predict_two * (even + ahead(even))
    even = even + update_two * (odd + behind(odd))
    table = np.zeros((rows, 256))
    table[:length, : length // 2] = even * scaling
    table[:length, 128 : 128 + length // 2] = odd / scaling
    one = table.astype(np.float32).astype(BF16)
    two = (table - one.astype(np.float64)).astype(np.float32).astype(BF16)
    return np.concatenate([one, two, one], axis=0)


class Lift:
    def __init__(self, cell):
        self.cell = cell
        self.known = {}

    def get(self, key, make):
        if key not in self.known:
            self.known[key] = make()
        return self.known[key]

    def even(self, i):
        return self.get(("e", i), lambda: self.cell(2 * i))

    def odd(self, i):
        return self.get(("o", i), lambda: self.cell(2 * i + 1))

    def odd_one(self, i):
        return self.get(("o1", i), lambda: self.odd(i) + predict_one * (self.even(i) + self.even(i + 1)))

    def even_one(self, i):
        return self.get(("e1", i), lambda: self.even(i) + update_one * (self.odd_one(i - 1) + self.odd_one(i)))

    def high(self, i):
        return self.get(("o2", i), lambda: self.odd_one(i) + predict_two * (self.even_one(i) + self.even_one(i + 1)))

    def low(self, i):
        return self.get(("e2", i), lambda: self.even_one(i) + update_two * (self.high(i - 1) + self.high(i)))


def loop(count, body):
    def step(i, carry):
        body(i)
        return carry

    lax.fori_loop(0, count, step, 0)


def along_y(load, x_high, wanted, put):
    lift = Lift(load)
    for y_high, j in wanted:
        value = lift.high(j) if y_high else lift.low(j)
        if x_high == y_high:
            value = value * (scaling**-2 if x_high else scaling**2)
        put(y_high, j, value)


def along_z(rows, table):
    high = rows.astype(BF16)
    rest = (rows - high.astype(F32)).astype(BF16)
    left = jnp.concatenate([high, high, rest], axis=1)
    return jnp.dot(left, table[...], preferred_element_type=F32)


def kernel(count_x, count_y, v, t1, t2, t3, d1, s1, d2, s2, d3, s3, coarse,
           cells, inner, outer, mixed, second, third, last, stage, w1, w2, w3,
           cs1, cr1, cs2, cr2, cs3, cr3, bands_low, own_sem, send_sem, recv_sem):
    gx, gy = lax.axis_index("gx"), lax.axis_index("gy")
    right, left = lax.rem(gx + 1, count_x), lax.rem(gx + count_x - 1, count_x)
    up, down = lax.rem(gy + 1, count_y), lax.rem(gy + count_y - 1, count_y)
    corners = ((right, up), (right, down), (left, up), (left, down))
    around = ((right, gy), (left, gy), (gx, up), (gx, down)) + corners

    own = [pltpu.make_async_copy(v.at[c], cells.at[c, 4:20, 8:72, :], own_sem.at[c]) for c in range(3)]
    tables = [pltpu.make_async_copy(src, dst, own_sem.at[3 + n]) for n, (src, dst) in enumerate(((t1, w1), (t2, w2), (t3, w3)))]
    for copy in own:
        copy.start()
    barrier = pltpu.get_barrier_semaphore()
    for device in around:
        pl.semaphore_signal(barrier, inc=1, device_id=device, device_id_type=MESH)
    for copy in tables:
        copy.start()
    pl.semaphore_wait(barrier, 8)

    started = []

    def send(src, dst, device):
        n = len(started)
        copy = pltpu.make_async_remote_copy(
            src_ref=src, dst_ref=dst, send_sem=send_sem.at[n], recv_sem=recv_sem.at[n], device_id=device, device_id_type=MESH
        )
        copy.start()
        started.append(copy)
        return copy

    def send_x(c):
        return (
            send(v.at[c, 12:16], cells.at[c, 0:4, 8:72, :], (right, gy)),
            send(v.at[c, 0:3], cells.at[c, 20:23, 8:72, :], (left, gy)),
        )

    x_halo = [send_x(0)]
    y_halo = (
        send(v.at[:, :, 56:64, :], cells.at[0:3, 4:20, 0:8, :], (gx, up)),
        send(v.at[:, :, 0:8, :], cells.at[0:3, 4:20, 72:80, :], (gx, down)),
    )
    for copy in own:
        copy.wait()
    for k, (layer, row) in enumerate(((16, 68), (16, 8), (4, 68), (4, 8))):
        for c in range(3):
            for m in range(2):
                for u in range(2):
                    cs1[k, c, m, 4 * u : 4 * u + 4, :] = cells[c, layer + 2 * m + u, row : row + 4, :]

    def fill(i):
        cells[3, i] = jnp.ones((80, 256), F32)

    loop(23, fill)
    corner_halo = [send(cs1.at[k], cr1.at[k], corners[k]) for k in range(4)]
    x_halo += [send_x(1), send_x(2)]
    for copy in tables:
        copy.wait()
    for copy in y_halo:
        copy.wait_recv()

    def index_of(g, t):
        return 3 + lax.div((t + 1) * (6 - t), 2) + g - (6 - t)

    def lift_x(g, t, wanted, put):
        other = lax.rem(t + 3, 4)

        def tile(i):
            rows = pl.ds(pl.multiple_of(i * 8, 8), 8)
            for h in range(2):
                lanes = slice(128 * h, 128 * h + 128)
                lift = Lift(lambda n: cells[g, 4 + n, rows, lanes] * cells[other, 4 + n, rows, lanes])
                for n, (x_high, k) in enumerate(wanted):
                    put(n, h, rows, lift.high(k) if x_high else lift.low(k))

        loop(10, tile)

    def lift_y(load, x_high, y_wanted, at):
        for h in range(2):
            for q in range(2):

                def put(y_high, j, value):
                    mixed[pl.ds(pl.multiple_of(at(y_high) + 16 * q + 8 * j, 8), 8), 128 * h : 128 * h + 128] = value

                wanted = [(y_high, j) for y_high in y_wanted for j in range(2)]
                along_y(lambda r: load(h, pl.ds(8 + 32 * q + r, 8, stride=4)), x_high, wanted, put)

    def lift_z(pieces):
        out = along_z(mixed[0 : 32 * len(pieces), :], w1)
        for n, (index, x_high, k, y_high) in enumerate(pieces):
            for q in range(2):
                for j in range(2):
                    at = 32 * n + 16 * q + 8 * j
                    for z_high in range(2):
                        value = out[at : at + 8, 128 * z_high : 128 * z_high + 128]
                        band = 4 * z_high + 2 * y_high + x_high
                        row = 16 * q + j
                        if band:
                            d1[band - 1, index, k, pl.ds(row, 8, stride=2), :] = value
                        else:
                            second[index, k, pl.ds(8 + row, 8, stride=2), :] = value

    inner_wanted = [(0, k) for k in (2, 3, 4, 5)] + [(1, k) for k in (1, 2, 3, 4, 5)]
    outer_wanted = [(0, k) for k in (0, 1, 6, 7)] + [(1, k) for k in (0, 6, 7)]

    def inner_field(g, t):
        def put(n, h, rows, value):
            inner[n, h, rows, :] = value

        lift_x(g, t, inner_wanted, put)

        def low(n):
            lift_y(lambda h, at: inner[n, h, at, :], 0, (0, 1), lambda y_high: n * 64 + 32 * y_high)

        def high(n):
            lift_y(lambda h, at: inner[4 + n, h, at, :], 1, (0, 1), lambda y_high: (4 + n) * 64 + 32 * y_high)

        loop(4, low)
        loop(5, high)
        lift_z([(index_of(g, t), x_high, k, y_high) for x_high, k in inner_wanted for y_high in range(2)])

    for g in range(3):
        loop(g + 2, lambda t: inner_field(g, t))

    for g in range(3):
        for copy in x_halo[g]:
            copy.wait_recv()
        if g == 0:
            for copy in corner_halo:
                copy.wait_recv()
            for k, (layer, row) in enumerate(((0, 4), (0, 72), (20, 4), (20, 72))):
                for c in range(3):
                    for m in range(2):
                        for u in range(2):
                            if layer + 2 * m + u < 23:
                                cells[c, layer + 2 * m + u, row : row + 4, :] = cr1[k, c, m, 4 * u : 4 * u + 4, :]

        def outer_field(t):
            index = index_of(g, t)

            def put(n, h, rows, value):
                outer[index, n, h, rows, :] = value

            lift_x(g, t, outer_wanted, put)

            def low(n):
                lift_y(lambda h, at: outer[index, n, h, at, :], 0, (0,), lambda y_high: t * 128 + n * 32)

            loop(4, low)

        loop(g + 2, outer_field)
        lift_z([(3 + (t + 1) * (6 - t) // 2 + g - (6 - t), x_high, k, 0) for t in range(g + 2) for x_high, k in outer_wanted[:4]])

    def outer_details(index):
        def low(n):
            lift_y(lambda h, at: outer[index, n, h, at, :], 0, (1,), lambda y_high: n * 32)

        def high(n):
            lift_y(lambda h, at: outer[index, 4 + n, h, at, :], 1, (0, 1), lambda y_high: 128 + n * 64 + 32 * y_high)

        loop(4, low)
        loop(3, high)
        pieces = [(index, x_high, k, 1) for x_high, k in outer_wanted[:4]]
        lift_z(pieces + [(index, x_high, k, y_high) for x_high, k in outer_wanted[4:] for y_high in range(2)])

    def exchange(field, n, rows, cs, cr):
        def prepare(f):
            def tile(i):
                at = pl.ds(pl.multiple_of(8 + i * 8, 8), 8)
                layer = lambda l: field[f, l, at, :]
                field[f, n + 4, at, :] = layer(n - 1) + predict_one * layer(n - 2)
                before = layer(n - 3) + predict_one * (layer(n - 4) + layer(n - 2))
                field[f, n + 5, at, :] = layer(n - 2) + update_one * before
                field[f, n + 6, at, :] = layer(0)
                field[f, n + 7, at, :] = layer(1) + predict_one * (layer(0) + layer(2))

            for i in range(rows // 8):
                tile(i)
            for k, (layer, row) in enumerate(((n + 4, 4 + rows), (n + 4, 8), (n + 6, 4 + rows), (n + 6, 8))):
                for u in range(2):
                    cs[k, f, 4 * u : 4 * u + 4, :] = field[f, layer + u, row : row + 4, :]

        loop(9, prepare)
        whole = slice(8, 8 + rows)
        halo = [
            send(field.at[:, n + 4 : n + 6, whole, :], field.at[:, n : n + 2, whole, :], (right, gy)),
            send(field.at[:, n + 6 : n + 8, whole, :], field.at[:, n + 2 : n + 4, whole, :], (left, gy)),
        ]
        halo += [send(cs.at[k], cr.at[k], corners[k]) for k in range(4)]
        halo += [
            send(field.at[:, 0:n, rows : rows + 8, :], field.at[:, 0:n, 0:8, :], (gx, up)),
            send(field.at[:, 0:n, 8:16, :], field.at[:, 0:n, 8 + rows : 16 + rows, :], (gx, down)),
        ]

        def finish():
            for copy in halo:
                copy.wait_recv()

            def unpack(f):
                for k, (layer, row) in enumerate(((n, 4), (n, 8 + rows), (n + 2, 4), (n + 2, 8 + rows))):
                    for u in range(2):
                        field[f, layer + u, row : row + 4, :] = cr[k, f, 4 * u : 4 * u + 4, :]

            loop(9, unpack)

        return finish

    def stresses(target, field, n, at):
        def layer(l):
            for k, (p, q) in enumerate(product_pairs):
                value = field[3 + k, l, at, :] - field[p, l, at, :] * field[q, l, at, :]
                target[k, l] = value[:, : target.shape[3]]

        loop(n, layer)

    def level(field, n, rows, table, put):
        half = n // 2
        block = rows // 8

        def one_field(f):
            def along_x(i):
                at = pl.ds(pl.multiple_of(i * 8, 8), 8)
                lift = Lift(lambda l: field[f, l if l < n else n + 2, at, :])
                lift.known[("o1", -1)] = field[f, n, at, :] + predict_one * lift.even(0)
                lift.known[("e1", -1)] = field[f, n + 1, at, :] + update_one * lift.odd_one(-1)
                lift.known[("o1", half)] = field[f, n + 3, at, :]
                lift.known[("o2", -1)] = lift.odd_one(-1) + predict_two * (lift.even_one(-1) + lift.even_one(0))
                for k in range(half):
                    bands_low[k, at, :] = lift.low(k)
                    bands_low[half + k, at, :] = lift.high(k)

            loop(rows // 8 + 2, along_x)

            wanted = [(y_high, j) for y_high in range(2) for j in range(block // 2)]

            def y_band(x_high):
                def one(k):
                    k = k + half if x_high else k

                    def put_row(y_high, j, value):
                        at = k * rows + y_high * (rows // 2) + j * 8
                        mixed[pl.ds(pl.multiple_of(at, 8), 8), 0:128] = value

                    along_y(lambda r: bands_low[k, pl.ds(8 + r, 8, stride=block), :], x_high, wanted, put_row)

                return one

            loop(half, y_band(0))
            loop(half, y_band(1))
            out = along_z(mixed[0 : n * rows, 0:128], table)
            for k in range(n):
                x_high, x_at = divmod(k, half)
                for y_high in range(2):
                    for j in range(block // 2):
                        at = k * rows + y_high * (rows // 2) + j * 8
                        for z_high in range(2):
                            value = out[at : at + 8, 128 * z_high : 128 * z_high + 128]
                            put(f, 4 * z_high + 2 * y_high + x_high, x_at, j, value)

        loop(9, one_field)

    finish = exchange(second, 8, 32, cs2, cr2)
    stresses(s1, second, 8, slice(8, 40))
    loop(9, outer_details)
    finish()

    def put_two(f, band, k, j, value):
        if band:
            stage[band - 1, k, pl.ds(j, 8, stride=2), :] = value
            if j == 1:
                d2[band - 1, f, k] = stage[band - 1, k][:, :64]
        else:
            third[f, k, pl.ds(8 + j, 8, stride=2), :] = value

    level(second, 8, 32, w2, put_two)
    finish = exchange(third, 4, 16, cs3, cr3)
    stresses(s2, third, 4, slice(8, 24))
    finish()

    def put_three(f, band, k, j, value):
        if band:
            d3[band - 1, f, k] = value[:, :32]
        else:
            last[f, k] = value

    level(third, 4, 16, w3, put_three)
    stresses(s3, last, 2, slice(0, 8))
    for c in range(3):
        coarse[c] = last[c][:, :, :32]
    for copy in started:
        copy.wait_send()


def flush(*refs):
    copies = [pltpu.make_async_copy(refs[n], refs[7 + n], refs[14].at[n]) for n in range(7)]
    for copy in copies:
        copy.start()
    for copy in copies:
        copy.wait()


def body(velocity):
    shapes = ((7, 9, 8, 32, 128), (6, 8, 32, 128), (7, 9, 4, 16, 64), (6, 4, 16, 64), (7, 9, 2, 8, 32), (6, 2, 8, 32), (3, 2, 8, 32))
    copies = 12 + 8 + 8
    limit = 50_000_000
    run = pl.pallas_call(
        lambda *refs: kernel(lax.axis_size("gx"), lax.axis_size("gy"), *refs),
        out_shape=[pltpu.VMEM(shape, F32) for shape in shapes],
        in_specs=[pl.BlockSpec(memory_space=pltpu.HBM)] * 4,
        out_specs=[pl.BlockSpec(memory_space=pltpu.VMEM)] * 7,
        scratch_shapes=[
            pltpu.VMEM((4, 23, 80, 256), F32),
            pltpu.VMEM((9, 2, 80, 128), F32),
            pltpu.VMEM((9, 7, 2, 80, 128), F32),
            pltpu.VMEM((576, 256), F32),
            pltpu.VMEM((9, 16, 48, 128), F32),
            pltpu.VMEM((9, 12, 32, 128), F32),
            pltpu.VMEM((9, 2, 8, 128), F32),
            pltpu.VMEM((7, 4, 16, 128), F32),
            pltpu.VMEM((768, 256), BF16),
            pltpu.VMEM((384, 256), BF16),
            pltpu.VMEM((384, 256), BF16),
            pltpu.VMEM((4, 3, 2, 8, 256), F32),
            pltpu.VMEM((4, 3, 2, 8, 256), F32),
            pltpu.VMEM((4, 9, 8, 128), F32),
            pltpu.VMEM((4, 9, 8, 128), F32),
            pltpu.VMEM((4, 9, 8, 128), F32),
            pltpu.VMEM((4, 9, 8, 128), F32),
            pltpu.VMEM((8, 48, 128), F32),
            pltpu.SemaphoreType.DMA((6,)),
            pltpu.SemaphoreType.DMA((copies,)),
            pltpu.SemaphoreType.DMA((copies,)),
        ],
        compiler_params=pltpu.CompilerParams(collective_id=0, has_side_effects=True, vmem_limit_bytes=limit),
    )
    results = run(velocity, third_table(256, 256), third_table(128, 128), third_table(64, 128))
    return tuple(
        pl.pallas_call(
            flush,
            out_shape=[pltpu.HBM(shape, F32) for shape in shapes],
            in_specs=[pl.BlockSpec(memory_space=pl.ANY)] * 7,
            out_specs=[pl.BlockSpec(memory_space=pl.ANY)] * 7,
            scratch_shapes=[pltpu.SemaphoreType.DMA((7,))],
            compiler_params=pltpu.CompilerParams(vmem_limit_bytes=1_000_000),
        )(*results)
    )


def solution(mesh):
    in_specs = (P(None, "gx", "gy", None),)
    out_specs = (
        P(None, None, "gx", "gy", None),
        P(None, "gx", "gy", None),
        P(None, None, "gx", "gy", None),
        P(None, "gx", "gy", None),
        P(None, None, "gx", "gy", None),
        P(None, "gx", "gy", None),
        P(None, "gx", "gy", None),
    )
    return jax.shard_map(body, mesh=mesh, in_specs=in_specs, out_specs=out_specs, check_vma=False)
```

```python
import jax
import jax.numpy as jnp
import numpy as np
from jax import lax
from jax.experimental import pallas as pl
from jax.experimental.pallas import tpu as pltpu
from jax.sharding import PartitionSpec as P

MESH = pl.DeviceIdType.MESH
F32 = jnp.float32
BF16 = jnp.bfloat16

predict_one = -1.586134342
update_one = -0.05298011854
predict_two = 0.8829110762
update_two = 0.4435068522
scaling = 1.149604398
product_pairs = ((0, 0), (0, 1), (0, 2), (1, 1), (1, 2), (2, 2))


def three_products(table, axis):
    one = table.astype(np.float32).astype(BF16)
    two = (table - one.astype(np.float64)).astype(np.float32).astype(BF16)
    return np.concatenate([one, two, one] if axis == 0 else [one, one, two], axis=axis)


def lift_table(cells, ahead, behind):
    even, odd = cells[0::2], cells[1::2]
    odd = odd + predict_one * (even + ahead(even))
    even = even + update_one * (odd + behind(odd))
    odd = odd + predict_two * (even + ahead(even))
    even = even + update_two * (odd + behind(odd))
    return even, odd


def third_table(length, rows):
    even, odd = lift_table(
        np.eye(length), lambda v: np.concatenate([v[1:], v[-1:]]), lambda v: np.concatenate([v[:1], v[:-1]])
    )
    table = np.zeros((rows, 256))
    table[:length, : length // 2] = even.T * scaling
    table[:length, 128 : 128 + length // 2] = odd.T / scaling
    return three_products(table, 0)


def second_table(rows, depth):
    even, odd = lift_table(
        np.eye(rows + 16), lambda v: np.concatenate([v[1:], v[-1:]]), lambda v: np.concatenate([v[:1], v[:-1]])
    )
    low, high = even[4 : 4 + rows // 2], odd[4 : 4 + rows // 2]
    tables = []
    for low_scale, high_scale in ((scaling**2, 1.0), (1.0, scaling**-2)):
        parts = three_products(np.concatenate([low * low_scale, high * high_scale]), 1)
        tables.append(np.concatenate([parts, np.zeros((rows, depth - parts.shape[1]), BF16)], axis=1))
    return np.stack(tables)


class Lift:
    def __init__(self, cell):
        self.cell = cell
        self.known = {}

    def get(self, key, make):
        if key not in self.known:
            self.known[key] = make()
        return self.known[key]

    def even(self, i):
        return self.get(("e", i), lambda: self.cell(2 * i))

    def odd(self, i):
        return self.get(("o", i), lambda: self.cell(2 * i + 1))

    def odd_one(self, i):
        return self.get(("o1", i), lambda: self.odd(i) + predict_one * (self.even(i) + self.even(i + 1)))

    def even_one(self, i):
        return self.get(("e1", i), lambda: self.even(i) + update_one * (self.odd_one(i - 1) + self.odd_one(i)))

    def high(self, i):
        return self.get(("o2", i), lambda: self.odd_one(i) + predict_two * (self.even_one(i) + self.even_one(i + 1)))

    def low(self, i):
        return self.get(("e2", i), lambda: self.even_one(i) + update_two * (self.high(i - 1) + self.high(i)))


def loop(count, body):
    def step(i, carry):
        body(i)
        return carry

    lax.fori_loop(0, count, step, 0)


def along_y(table, rows):
    high = rows.astype(BF16)
    rest = (rows - high.astype(F32)).astype(BF16)
    pad = table.shape[1] - 3 * rows.shape[0]
    right = jnp.concatenate([high, rest, high] + ([high[:pad]] if pad else []), axis=0)
    return jnp.dot(table, right, preferred_element_type=F32)


def along_z(rows, table):
    high = rows.astype(BF16)
    rest = (rows - high.astype(F32)).astype(BF16)
    left = jnp.concatenate([high, high, rest], axis=1)
    return jnp.dot(left, table[...], preferred_element_type=F32)


def kernel(count_x, count_y, v, z1, z2, z3, y1, y2, y3, d1, s1, d2, s2, d3, s3, coarse,
           cells, inner, outer, mixed, second, third, last, wz1, wz2, wz3, wy1, wy2, wy3,
           cs1, cr1, cs2, cr2, cs3, cr3, bands, own_sem, send_sem, recv_sem):
    gx, gy = lax.axis_index("gx"), lax.axis_index("gy")
    right, left = lax.rem(gx + 1, count_x), lax.rem(gx + count_x - 1, count_x)
    up, down = lax.rem(gy + 1, count_y), lax.rem(gy + count_y - 1, count_y)
    corners = ((right, up), (right, down), (left, up), (left, down))
    around = ((right, gy), (left, gy), (gx, up), (gx, down)) + corners

    own = [pltpu.make_async_copy(v.at[c], cells.at[c, 4:20, 8:72, :], own_sem.at[c]) for c in range(3)]
    pairs = ((z1, wz1), (z2, wz2), (z3, wz3), (y1, wy1), (y2, wy2), (y3, wy3))
    tables = [pltpu.make_async_copy(src, dst, own_sem.at[3 + n]) for n, (src, dst) in enumerate(pairs)]
    barrier = pltpu.get_barrier_semaphore()
    for device in around:
        pl.semaphore_signal(barrier, inc=1, device_id=device, device_id_type=MESH)
    for copy in own + tables:
        copy.start()
    pl.semaphore_wait(barrier, 8)

    started = []

    def send(src, dst, device):
        n = len(started)
        copy = pltpu.make_async_remote_copy(
            src_ref=src, dst_ref=dst, send_sem=send_sem.at[n], recv_sem=recv_sem.at[n], device_id=device, device_id_type=MESH
        )
        copy.start()
        started.append(copy)
        return copy

    def send_x(c):
        return (
            send(v.at[c, 12:16], cells.at[c, 0:4, 8:72, :], (right, gy)),
            send(v.at[c, 0:3], cells.at[c, 20:23, 8:72, :], (left, gy)),
        )

    def index_of(g, t):
        return 3 + ((t + 1) * (6 - t)) // 2 + g - (6 - t)

    slots = {index_of(g, t): (0, 2, 5)[g] + t for g in range(3) for t in range(g + 2)}

    x_halo = [send_x(0)]
    y_halo = (
        send(v.at[:, :, 56:64, :], cells.at[0:3, 4:20, 0:8, :], (gx, up)),
        send(v.at[:, :, 0:8, :], cells.at[0:3, 4:20, 72:80, :], (gx, down)),
    )
    for copy in own:
        copy.wait()
    for k, (layer, row) in enumerate(((16, 68), (16, 8), (4, 68), (4, 8))):
        for c in range(3):
            for m in range(2):
                for u in range(2):
                    cs1[k, c, m, 4 * u : 4 * u + 4, :] = cells[c, layer + 2 * m + u, row : row + 4, :]

    def fill(i):
        cells[3, i] = jnp.ones((80, 256), F32)

    loop(23, fill)
    corner_halo = [send(cs1.at[k], cr1.at[k], corners[k]) for k in range(4)]
    x_halo += [send_x(1), send_x(2)]
    for row in (0, 72):
        for layer in (0, 1, 2, 3, 20, 21, 22):
            for c in range(3):
                cells[c, layer, row : row + 8, :] = jnp.zeros((8, 256), F32)
    for f in range(9):
        for layer in range(8, 12):
            for row in (0, 40):
                second[f, layer, row : row + 8, :] = jnp.zeros((8, 128), F32)
        for layer in range(4, 6):
            for row in (0, 24):
                third[f, layer, row : row + 8, :] = jnp.zeros((8, 128), F32)
    for copy in tables:
        copy.wait()
    for copy in y_halo:
        copy.wait_recv()

    def lift_x(g, t, wanted, put):
        other = lax.rem(t + 3, 4)

        def tile(i):
            rows = pl.ds(pl.multiple_of(i * 8, 8), 8)
            for h in range(2):
                lanes = slice(128 * h, 128 * h + 128)
                lift = Lift(lambda n: cells[g, 4 + n, rows, lanes] * cells[other, 4 + n, rows, lanes])
                for n, (x_high, k) in enumerate(wanted):
                    put(n, rows, lanes, lift.high(k) if x_high else lift.low(k))

        loop(10, tile)

    def lift_z(pieces):
        out = along_z(mixed[0 : 32 * len(pieces), :], wz1)
        for n, (index, slot, x_high, k, y_high) in enumerate(pieces):
            for z_high in range(2):
                value = out[32 * n : 32 * n + 32, 128 * z_high : 128 * z_high + 128]
                band = 4 * z_high + 2 * y_high + x_high
                if band:
                    d1[band - 1, index, k] = value
                else:
                    second[slot, k, 8:40, :] = value

    inner_wanted = [(0, k) for k in (2, 3, 4, 5)] + [(1, k) for k in (1, 2, 3, 4, 5)]
    outer_wanted = [(0, k) for k in (0, 1, 6, 7)] + [(1, k) for k in (0, 6, 7)]

    def inner_field(g, t):
        index = 3 + lax.div((t + 1) * (6 - t), 2) + g - (6 - t)

        def put(n, rows, lanes, value):
            inner[n, rows, lanes] = value

        lift_x(g, t, inner_wanted, put)
        for n, (x_high, k) in enumerate(inner_wanted):
            mixed[n * 64 : n * 64 + 64, :] = along_y(wy1[x_high], inner[n])
        lift_z([(index, (0, 2, 5)[g] + t, x_high, k, y_high) for x_high, k in inner_wanted for y_high in range(2)])

    def outer_group(g):
        for copy in x_halo[g]:
            copy.wait_recv()
        if g == 0:
            for copy in corner_halo:
                copy.wait_recv()
            for k, (layer, row) in enumerate(((0, 4), (0, 72), (20, 4), (20, 72))):
                for c in range(3):
                    for m in range(2):
                        for u in range(2):
                            if layer + 2 * m + u < 23:
                                cells[c, layer + 2 * m + u, row : row + 4, :] = cr1[k, c, m, 4 * u : 4 * u + 4, :]
        base = (0, 2, 5)[g]

        def outer_field(t):
            slot = base + t

            def put(n, rows, lanes, value):
                outer[slot, n, rows, lanes] = value

            lift_x(g, t, outer_wanted, put)
            for n in range(4):
                at = pl.ds(pl.multiple_of(t * 128 + n * 32, 32), 32)
                mixed[at, :] = along_y(wy1[0, 0:32], outer[slot, n])

        loop(g + 2, outer_field)
        lift_z([(index_of(g, t), base + t, x_high, k, 0) for t in range(g + 2) for x_high, k in outer_wanted[:4]])

    def outer_details(g):
        def one(t):
            index = 3 + lax.div((t + 1) * (6 - t), 2) + g - (6 - t)
            slot = (0, 2, 5)[g] + t
            for n in range(4):
                mixed[n * 32 : n * 32 + 32, :] = along_y(wy1[0, 32:64], outer[slot, n])
            for n in range(3):
                mixed[128 + n * 64 : 192 + n * 64, :] = along_y(wy1[1], outer[slot, 4 + n])
            pieces = [(index, slot, x_high, k, 1) for x_high, k in outer_wanted[:4]]
            lift_z(pieces + [(index, slot, x_high, k, y_high) for x_high, k in outer_wanted[4:] for y_high in range(2)])

        loop(g + 2, one)

    def exchange_two(g):
        n, rows, field = 8, 32, second
        at_group = pl.ds((0, 2, 5)[g], g + 2)

        def prepare(t):
            f = (0, 2, 5)[g] + t
            for i in range(rows // 8):
                at = pl.ds(8 + i * 8, 8)
                layer = lambda l: field[f, l, at, :]
                field[f, n + 4, at, :] = layer(n - 1) + predict_one * layer(n - 2)
                before = layer(n - 3) + predict_one * (layer(n - 4) + layer(n - 2))
                field[f, n + 5, at, :] = layer(n - 2) + update_one * before
                field[f, n + 6, at, :] = layer(0)
                field[f, n + 7, at, :] = layer(1) + predict_one * (layer(0) + layer(2))
            for k, (layer, row) in enumerate(((n + 4, 4 + rows), (n + 4, 8), (n + 6, 4 + rows), (n + 6, 8))):
                for u in range(2):
                    cs2[k, f, 4 * u : 4 * u + 4, :] = field[f, layer + u, row : row + 4, :]

        loop(g + 2, prepare)
        whole = slice(8, 8 + rows)
        halo = [
            send(field.at[at_group, n + 4 : n + 6, whole, :], field.at[at_group, n : n + 2, whole, :], (right, gy)),
            send(field.at[at_group, n + 6 : n + 8, whole, :], field.at[at_group, n + 2 : n + 4, whole, :], (left, gy)),
        ]
        halo += [send(cs2.at[k, at_group], cr2.at[k, at_group], corners[k]) for k in range(4)]
        halo += [
            send(field.at[at_group, 0:n, rows : rows + 8, :], field.at[at_group, 0:n, 0:8, :], (gx, up)),
            send(field.at[at_group, 0:n, 8:16, :], field.at[at_group, 0:n, 8 + rows : 16 + rows, :], (gx, down)),
        ]

        def finish():
            for copy in halo:
                copy.wait_recv()
            for t in range(g + 2):
                f = (0, 2, 5)[g] + t
                for k, (layer, row) in enumerate(((n, 4), (n, 8 + rows), (n + 2, 4), (n + 2, 8 + rows))):
                    for u in range(2):
                        field[f, layer + u, row : row + 4, :] = cr2[k, f, 4 * u : 4 * u + 4, :]

        return finish

    def exchange_three(g):
        n, rows, field = 4, 16, third
        at_group = pl.ds((0, 2, 5)[g], g + 2)
        at_pairs = pl.ds((0, 1, 3)[g], (1, 2, 2)[g])
        for t in range(g + 2):
            f = (0, 2, 5)[g] + t
            for i in range(rows // 8):
                at = pl.ds(8 + i * 8, 8)
                layer = lambda l: field[f, l, at, :]
                before = layer(1) + predict_one * (layer(0) + layer(2))
                p, q = layer(3) + predict_one * layer(2), layer(2) + update_one * before
                field[f, 6, at, :] = p + pltpu.roll(q, 64, 1)
                field[f, 7, at, :] = layer(0) + pltpu.roll(before, 64, 1)
            pair, half = (0, 1, 3)[g] + t // 2, 4 * (t % 2)
            for k, (layer, row) in enumerate(((6, 4 + rows), (6, 8), (7, 4 + rows), (7, 8))):
                cs3[k, pair, half : half + 4, :] = field[f, layer, row : row + 4, :]
        whole = slice(8, 8 + rows)
        halo = [
            send(field.at[at_group, 6:7, whole, :], field.at[at_group, 4:5, whole, :], (right, gy)),
            send(field.at[at_group, 7:8, whole, :], field.at[at_group, 5:6, whole, :], (left, gy)),
        ]
        halo += [send(cs3.at[k, at_pairs], cr3.at[k, at_pairs], corners[k]) for k in range(4)]
        halo += [
            send(field.at[at_group, 0:n, rows : rows + 8, :], field.at[at_group, 0:n, 0:8, :], (gx, up)),
            send(field.at[at_group, 0:n, 8:16, :], field.at[at_group, 0:n, 8 + rows : 16 + rows, :], (gx, down)),
        ]

        def finish():
            for copy in halo:
                copy.wait_recv()
            for t in range(g + 2):
                f, pair, half = (0, 2, 5)[g] + t, (0, 1, 3)[g] + t // 2, 4 * (t % 2)
                for k, (layer, row) in enumerate(((4, 4), (4, 8 + rows), (5, 4), (5, 8 + rows))):
                    field[f, layer, row : row + 4, :] = cr3[k, pair, half : half + 4, :]

        return finish

    def stresses(target, field, n, at):
        def layer(l):
            for k, (p, q) in enumerate(product_pairs):
                value = field[slots[3 + k], l, at, :] - field[slots[p], l, at, :] * field[slots[q], l, at, :]
                target[k, l] = value[:, : target.shape[3]]

        loop(n, layer)

    def level(g, field, n, rows, halo_of, wy, wz, put):
        half = n // 2

        def one_field(t):
            slot = (0, 2, 5)[g] + t
            index = 3 + lax.div((t + 1) * (6 - t), 2) + g - (6 - t)

            def along_x(i):
                at = pl.ds(pl.multiple_of(i * 8, 8), 8)
                p, q, next_even, next_odd = halo_of(slot, at)
                lift = Lift(lambda l: field[slot, l, at, :] if l < n else next_even)
                lift.known[("o1", -1)] = p + predict_one * lift.even(0)
                lift.known[("e1", -1)] = q + update_one * lift.odd_one(-1)
                lift.known[("o1", half)] = next_odd
                for k in range(half):
                    bands[k, at, :] = lift.low(k)
                    bands[half + k, at, :] = lift.high(k)

            loop(rows // 8 + 2, along_x)
            whole = rows + 16
            for k in range(0, n, 2):
                two = jnp.concatenate([bands[k, 0:whole, :], bands[k + 1, 0:whole, :]], axis=1)
                out = along_y(wy[k // half], two)
                mixed[k * rows : k * rows + rows, 0:128] = out[:, :128]
                mixed[k * rows + rows : k * rows + 2 * rows, 0:128] = out[:, 128:]
            out = along_z(mixed[0 : n * rows, 0:128], wz)
            for k in range(n):
                x_high, x_at = divmod(k, half)
                for y_high in range(2):
                    at = k * rows + y_high * (rows // 2)
                    for z_high in range(2):
                        value = out[at : at + rows // 2, 128 * z_high : 128 * z_high + 128]
                        put(index, slot, 4 * z_high + 2 * y_high + x_high, x_at, value)

        loop(g + 2, one_field)

    def halo_two(slot, at):
        return tuple(second[slot, 8 + l, at, :] for l in range(4))

    def put_two(index, slot, band, k, value):
        if band:
            d2[band - 1, index, k] = value[:, :64]
        else:
            third[slot, k, 8:24, :] = value

    def halo_three(slot, at):
        before, after = third[slot, 4, at, :], third[slot, 5, at, :]
        return before, pltpu.roll(before, 64, 1), after, pltpu.roll(after, 64, 1)

    def put_three(index, slot, band, k, value):
        if band:
            d3[band - 1, index, k] = value[:, :32]
        else:
            last[slot, k] = value

    for g in range(3):
        loop(g + 2, lambda t: inner_field(g, t))
    finish_two = []
    for g in range(3):
        outer_group(g)
        finish_two.append(exchange_two(g))
    for g in range(3):
        outer_details(g)
    stresses(s1, second, 8, slice(8, 40))
    finish_three = []
    for g in range(3):
        finish_two[g]()
        level(g, second, 8, 32, halo_two, wy2, wz2, put_two)
        finish_three.append(exchange_three(g))
    stresses(s2, third, 4, slice(8, 24))
    for g in range(3):
        finish_three[g]()
        level(g, third, 4, 16, halo_three, wy3, wz3, put_three)
    stresses(s3, last, 2, slice(0, 8))
    for c in range(3):
        coarse[c] = last[slots[c]][:, :, :32]
    for copy in started:
        copy.wait_send()


def flush(*refs):
    copies = [pltpu.make_async_copy(refs[n], refs[7 + n], refs[14].at[n]) for n in range(7)]
    for copy in copies:
        copy.start()
    for copy in copies:
        copy.wait()


def body(velocity):
    shapes = ((7, 9, 8, 32, 128), (6, 8, 32, 128), (7, 9, 4, 16, 64), (6, 4, 16, 64), (7, 9, 2, 8, 32), (6, 2, 8, 32), (3, 2, 8, 32))
    copies = 12 + 24 + 24
    limit = 50_000_000
    run = pl.pallas_call(
        lambda *refs: kernel(lax.axis_size("gx"), lax.axis_size("gy"), *refs),
        out_shape=[pltpu.VMEM(shape, F32) for shape in shapes],
        in_specs=[pl.BlockSpec(memory_space=pltpu.HBM)] * 7,
        out_specs=[pl.BlockSpec(memory_space=pltpu.VMEM)] * 7,
        scratch_shapes=[
            pltpu.VMEM((4, 23, 80, 256), F32),
            pltpu.VMEM((9, 80, 256), F32),
            pltpu.VMEM((9, 7, 80, 256), F32),
            pltpu.VMEM((576, 256), F32),
            pltpu.VMEM((9, 16, 48, 128), F32),
            pltpu.VMEM((9, 8, 32, 128), F32),
            pltpu.VMEM((9, 2, 8, 128), F32),
            pltpu.VMEM((768, 256), BF16),
            pltpu.VMEM((384, 256), BF16),
            pltpu.VMEM((384, 256), BF16),
            pltpu.VMEM((2, 64, 256), BF16),
            pltpu.VMEM((2, 32, 144), BF16),
            pltpu.VMEM((2, 16, 96), BF16),
            pltpu.VMEM((4, 3, 2, 8, 256), F32),
            pltpu.VMEM((4, 3, 2, 8, 256), F32),
            pltpu.VMEM((4, 9, 8, 128), F32),
            pltpu.VMEM((4, 9, 8, 128), F32),
            pltpu.VMEM((4, 5, 8, 128), F32),
            pltpu.VMEM((4, 5, 8, 128), F32),
            pltpu.VMEM((8, 48, 128), F32),
            pltpu.SemaphoreType.DMA((9,)),
            pltpu.SemaphoreType.DMA((copies,)),
            pltpu.SemaphoreType.DMA((copies,)),
        ],
        compiler_params=pltpu.CompilerParams(collective_id=0, has_side_effects=True, vmem_limit_bytes=limit),
    )
    along_third = (third_table(256, 256), third_table(128, 128), third_table(64, 128))
    along_second = (second_table(64, 256), second_table(32, 144), second_table(16, 96))
    results = run(velocity, *along_third, *along_second)
    return tuple(
        pl.pallas_call(
            flush,
            out_shape=[pltpu.HBM(shape, F32) for shape in shapes],
            in_specs=[pl.BlockSpec(memory_space=pl.ANY)] * 7,
            out_specs=[pl.BlockSpec(memory_space=pl.ANY)] * 7,
            scratch_shapes=[pltpu.SemaphoreType.DMA((7,))],
            compiler_params=pltpu.CompilerParams(vmem_limit_bytes=1_000_000),
        )(*results)
    )


def solution(mesh):
    in_specs = (P(None, "gx", "gy", None),)
    out_specs = (
        P(None, None, "gx", "gy", None),
        P(None, "gx", "gy", None),
        P(None, None, "gx", "gy", None),
        P(None, "gx", "gy", None),
        P(None, None, "gx", "gy", None),
        P(None, "gx", "gy", None),
        P(None, "gx", "gy", None),
    )
    return jax.shard_map(body, mesh=mesh, in_specs=in_specs, out_specs=out_specs, check_vma=False)
```

```python
import jax
import jax.numpy as jnp
import numpy as np
from jax import lax
from jax.experimental import pallas as pl
from jax.experimental.pallas import tpu as pltpu
from jax.sharding import PartitionSpec as P

MESH = pl.DeviceIdType.MESH
F32 = jnp.float32
BF16 = jnp.bfloat16

predict_one = -1.586134342
update_one = -0.05298011854
predict_two = 0.8829110762
update_two = 0.4435068522
scaling = 1.149604398
product_pairs = ((0, 0), (0, 1), (0, 2), (1, 1), (1, 2), (2, 2))


def three_products(table, axis):
    one = table.astype(np.float32).astype(BF16)
    two = (table - one.astype(np.float64)).astype(np.float32).astype(BF16)
    return np.concatenate([one, two, one] if axis == 0 else [one, one, two], axis=axis)


def lift_table(cells, ahead, behind):
    even, odd = cells[0::2], cells[1::2]
    odd = odd + predict_one * (even + ahead(even))
    even = even + update_one * (odd + behind(odd))
    odd = odd + predict_two * (even + ahead(even))
    even = even + update_two * (odd + behind(odd))
    return even, odd


def third_table(length, rows):
    even, odd = lift_table(
        np.eye(length), lambda v: np.concatenate([v[1:], v[-1:]]), lambda v: np.concatenate([v[:1], v[:-1]])
    )
    table = np.zeros((rows, 256))
    table[:length, : length // 2] = even.T * scaling
    table[:length, 128 : 128 + length // 2] = odd.T / scaling
    return three_products(table, 0)


def second_table(rows, depth):
    even, odd = lift_table(
        np.eye(rows + 16), lambda v: np.concatenate([v[1:], v[-1:]]), lambda v: np.concatenate([v[:1], v[:-1]])
    )
    low, high = even[4 : 4 + rows // 2], odd[4 : 4 + rows // 2]
    tables = []
    for low_scale, high_scale in ((scaling**2, 1.0), (1.0, scaling**-2)):
        parts = three_products(np.concatenate([low * low_scale, high * high_scale]), 1)
        tables.append(np.concatenate([parts, np.zeros((rows, depth - parts.shape[1]), BF16)], axis=1))
    return np.stack(tables)


class Lift:
    def __init__(self, cell):
        self.cell = cell
        self.known = {}

    def get(self, key, make):
        if key not in self.known:
            self.known[key] = make()
        return self.known[key]

    def even(self, i):
        return self.get(("e", i), lambda: self.cell(2 * i))

    def odd(self, i):
        return self.get(("o", i), lambda: self.cell(2 * i + 1))

    def odd_one(self, i):
        return self.get(("o1", i), lambda: self.odd(i) + predict_one * (self.even(i) + self.even(i + 1)))

    def even_one(self, i):
        return self.get(("e1", i), lambda: self.even(i) + update_one * (self.odd_one(i - 1) + self.odd_one(i)))

    def high(self, i):
        return self.get(("o2", i), lambda: self.odd_one(i) + predict_two * (self.even_one(i) + self.even_one(i + 1)))

    def low(self, i):
        return self.get(("e2", i), lambda: self.even_one(i) + update_two * (self.high(i - 1) + self.high(i)))


def loop(count, body):
    def step(i, carry):
        body(i)
        return carry

    lax.fori_loop(0, count, step, 0)


def along_y(table, rows):
    high = rows.astype(BF16)
    rest = (rows - high.astype(F32)).astype(BF16)
    pad = table.shape[1] - 3 * rows.shape[0]
    right = jnp.concatenate([high, rest, high] + ([high[:pad]] if pad else []), axis=0)
    return jnp.dot(table, right, preferred_element_type=F32)


def along_z(rows, table):
    high = rows.astype(BF16)
    rest = (rows - high.astype(F32)).astype(BF16)
    left = jnp.concatenate([high, high, rest], axis=1)
    return jnp.dot(left, table[...], preferred_element_type=F32)


def kernel(count_x, count_y, v, z1, z2, z3, y1, y2, y3, d1, s1, d2, s2, d3, s3, coarse,
           cells, inner, outer, mixed, second, third, last, wz1, wz2, wz3, wy1, wy2, wy3,
           cs1, cr1, cs2, cr2, cs3, cr3, bands, own_sem, send_sem, recv_sem):
    gx, gy = lax.axis_index("gx"), lax.axis_index("gy")
    right, left = lax.rem(gx + 1, count_x), lax.rem(gx + count_x - 1, count_x)
    up, down = lax.rem(gy + 1, count_y), lax.rem(gy + count_y - 1, count_y)
    corners = ((right, up), (right, down), (left, up), (left, down))
    around = ((right, gy), (left, gy), (gx, up), (gx, down)) + corners

    own = [pltpu.make_async_copy(v.at[c], cells.at[c, 4:20, 8:72, :], own_sem.at[c]) for c in range(3)]
    pairs = ((z1, wz1), (z2, wz2), (z3, wz3), (y1, wy1), (y2, wy2), (y3, wy3))
    tables = [pltpu.make_async_copy(src, dst, own_sem.at[3 + n]) for n, (src, dst) in enumerate(pairs)]
    barrier = pltpu.get_barrier_semaphore()
    for device in around:
        pl.semaphore_signal(barrier, inc=1, device_id=device, device_id_type=MESH)
    for copy in own + tables:
        copy.start()
    pl.semaphore_wait(barrier, 8)

    started = []

    def send(src, dst, device):
        n = len(started)
        copy = pltpu.make_async_remote_copy(
            src_ref=src, dst_ref=dst, send_sem=send_sem.at[n], recv_sem=recv_sem.at[n], device_id=device, device_id_type=MESH
        )
        copy.start()
        started.append(copy)
        return copy

    def send_x(c):
        return (
            send(v.at[c, 12:16], cells.at[c, 0:4, 8:72, :], (right, gy)),
            send(v.at[c, 0:3], cells.at[c, 20:23, 8:72, :], (left, gy)),
        )

    def index_of(g, t):
        return 3 + ((t + 1) * (6 - t)) // 2 + g - (6 - t)

    slots = {index_of(g, t): (0, 2, 5)[g] + t for g in range(3) for t in range(g + 2)}

    x_halo = [send_x(0)]
    y_halo = [
        (
            send(v.at[c, :, 56:64, :], cells.at[c, 4:20, 0:8, :], (gx, up)),
            send(v.at[c, :, 0:8, :], cells.at[c, 4:20, 72:80, :], (gx, down)),
        )
        for c in range(3)
    ]
    for copy in own:
        copy.wait()
    for k, (layer, row) in enumerate(((16, 68), (16, 8), (4, 68), (4, 8))):
        for c in range(3):
            for m in range(2):
                for u in range(2):
                    cs1[k, c, m, 4 * u : 4 * u + 4, :] = cells[c, layer + 2 * m + u, row : row + 4, :]

    def fill(i):
        cells[3, i] = jnp.ones((80, 256), F32)

    loop(23, fill)
    corner_halo = [send(cs1.at[k], cr1.at[k], corners[k]) for k in range(4)]
    x_halo += [send_x(1), send_x(2)]
    for row in (0, 72):
        for layer in (0, 1, 2, 3, 20, 21, 22):
            for c in range(3):
                cells[c, layer, row : row + 8, :] = jnp.zeros((8, 256), F32)
    for f in range(9):
        for layer in range(8, 12):
            for row in (0, 40):
                second[f, layer, row : row + 8, :] = jnp.zeros((8, 128), F32)
        for layer in range(4, 6):
            for row in (0, 24):
                third[f, layer, row : row + 8, :] = jnp.zeros((8, 128), F32)
    for copy in tables:
        copy.wait()

    def lift_x(g, t, wanted, put):
        other = lax.rem(t + 3, 4)

        def tile(i):
            rows = pl.ds(pl.multiple_of(i * 8, 8), 8)
            for h in range(2):
                lanes = slice(128 * h, 128 * h + 128)
                lift = Lift(lambda n: cells[g, 4 + n, rows, lanes] * cells[other, 4 + n, rows, lanes])
                for n, (x_high, k) in enumerate(wanted):
                    put(n, rows, lanes, lift.high(k) if x_high else lift.low(k))

        loop(10, tile)

    def lift_z(pieces):
        out = along_z(mixed[0 : 32 * len(pieces), :], wz1)
        for n, (index, slot, x_high, k, y_high) in enumerate(pieces):
            for z_high in range(2):
                value = out[32 * n : 32 * n + 32, 128 * z_high : 128 * z_high + 128]
                band = 4 * z_high + 2 * y_high + x_high
                if band:
                    d1[band - 1, index, k] = value
                else:
                    second[slot, k, 8:40, :] = value

    inner_wanted = [(0, k) for k in (2, 3, 4, 5)] + [(1, k) for k in (1, 2, 3, 4, 5)]
    outer_wanted = [(0, k) for k in (0, 1, 6, 7)] + [(1, k) for k in (0, 6, 7)]

    def inner_field(g, t):
        index = 3 + lax.div((t + 1) * (6 - t), 2) + g - (6 - t)

        def put(n, rows, lanes, value):
            inner[n, rows, lanes] = value

        lift_x(g, t, inner_wanted, put)
        for n, (x_high, k) in enumerate(inner_wanted):
            mixed[n * 64 : n * 64 + 64, :] = along_y(wy1[x_high], inner[n])
        lift_z([(index, (0, 2, 5)[g] + t, x_high, k, y_high) for x_high, k in inner_wanted for y_high in range(2)])

    sides = {"right": ((6, 7), (6, 7), 2, 5), "left": ((0, 1), (0,), 0, 4), "both": ((0, 1, 6, 7), (0, 6, 7), 0, 4)}

    def unpack_corners(which):
        for k in which:
            corner_halo[k].wait_recv()
            layer, row = ((0, 4), (0, 72), (20, 4), (20, 72))[k]
            for c in range(3):
                for m in range(2):
                    for u in range(2):
                        if layer + 2 * m + u < 23:
                            cells[c, layer + 2 * m + u, row : row + 4, :] = cr1[k, c, m, 4 * u : 4 * u + 4, :]

    def outer_group(g, side):
        lows, highs, low_at, high_at = sides[side]
        wanted = [(0, k) for k in lows] + [(1, k) for k in highs]
        places = [low_at + n for n in range(len(lows))] + [high_at + n for n in range(len(highs))]
        base = (0, 2, 5)[g]

        def outer_field(t):
            slot = base + t

            def put(n, rows, lanes, value):
                outer[slot, places[n], rows, lanes] = value

            lift_x(g, t, wanted, put)
            for n in range(len(lows)):
                at = pl.ds(pl.multiple_of(t * 32 * len(lows) + n * 32, 32), 32)
                mixed[at, :] = along_y(wy1[0, 0:32], outer[slot, low_at + n])

        loop(g + 2, outer_field)
        lift_z([(index_of(g, t), base + t, 0, k, 0) for t in range(g + 2) for k in lows])

    def outer_details(g, side):
        lows, highs, low_at, high_at = sides[side]

        def one(t):
            index = 3 + lax.div((t + 1) * (6 - t), 2) + g - (6 - t)
            slot = (0, 2, 5)[g] + t
            for n in range(len(lows)):
                mixed[n * 32 : n * 32 + 32, :] = along_y(wy1[0, 32:64], outer[slot, low_at + n])
            for n in range(len(highs)):
                at = 32 * len(lows) + n * 64
                mixed[at : at + 64, :] = along_y(wy1[1], outer[slot, high_at + n])
            pieces = [(index, slot, 0, k, 1) for k in lows]
            lift_z(pieces + [(index, slot, 1, k, y_high) for k in highs for y_high in range(2)])

        loop(g + 2, one)

    halo_of_two = {0: [], 1: [], 2: []}

    def send_two(g, side):
        n, rows, field = 8, 32, second
        base = (0, 2, 5)[g]
        at_group = pl.ds(base, g + 2)
        start = n + 4 if side == "right" else n + 6

        def prepare(t):
            f = base + t
            for i in range(rows // 8):
                at = pl.ds(8 + i * 8, 8)
                layer = lambda l: field[f, l, at, :]
                if side == "right":
                    field[f, start, at, :] = layer(n - 1) + predict_one * layer(n - 2)
                    before = layer(n - 3) + predict_one * (layer(n - 4) + layer(n - 2))
                    field[f, start + 1, at, :] = layer(n - 2) + update_one * before
                else:
                    field[f, start, at, :] = layer(0)
                    field[f, start + 1, at, :] = layer(1) + predict_one * (layer(0) + layer(2))
            for k, row in enumerate((4 + rows, 8)):
                k = k if side == "right" else k + 2
                for u in range(2):
                    cs2[k, f, 4 * u : 4 * u + 4, :] = field[f, start + u, row : row + 4, :]

        loop(g + 2, prepare)
        whole = slice(8, 8 + rows)
        to = start - 4
        device, first = ((right, gy), 0) if side == "right" else ((left, gy), 2)
        halo = [send(field.at[at_group, start : start + 2, whole, :], field.at[at_group, to : to + 2, whole, :], device)]
        halo += [send(cs2.at[k, at_group], cr2.at[k, at_group], corners[k]) for k in (first, first + 1)]
        if side == "left":
            halo += [
                send(field.at[at_group, 0:n, rows : rows + 8, :], field.at[at_group, 0:n, 0:8, :], (gx, up)),
                send(field.at[at_group, 0:n, 8:16, :], field.at[at_group, 0:n, 8 + rows : 16 + rows, :], (gx, down)),
            ]
        halo_of_two[g].extend(halo)

    def finish_two(g):
        n, rows, field = 8, 32, second
        for copy in halo_of_two[g]:
            copy.wait_recv()
        for t in range(g + 2):
            f = (0, 2, 5)[g] + t
            for k, (layer, row) in enumerate(((n, 4), (n, 8 + rows), (n + 2, 4), (n + 2, 8 + rows))):
                for u in range(2):
                    field[f, layer + u, row : row + 4, :] = cr2[k, f, 4 * u : 4 * u + 4, :]

    def exchange_three(g):
        n, rows, field = 4, 16, third
        at_group = pl.ds((0, 2, 5)[g], g + 2)
        at_pairs = pl.ds((0, 1, 3)[g], (1, 2, 2)[g])
        for t in range(g + 2):
            f = (0, 2, 5)[g] + t
            for i in range(rows // 8):
                at = pl.ds(8 + i * 8, 8)
                layer = lambda l: field[f, l, at, :]
                before = layer(1) + predict_one * (layer(0) + layer(2))
                p, q = layer(3) + predict_one * layer(2), layer(2) + update_one * before
                field[f, 6, at, :] = p + pltpu.roll(q, 64, 1)
                field[f, 7, at, :] = layer(0) + pltpu.roll(before, 64, 1)
            pair, half = (0, 1, 3)[g] + t // 2, 4 * (t % 2)
            for k, (layer, row) in enumerate(((6, 4 + rows), (6, 8), (7, 4 + rows), (7, 8))):
                cs3[k, pair, half : half + 4, :] = field[f, layer, row : row + 4, :]
        whole = slice(8, 8 + rows)
        halo = [
            send(field.at[at_group, 6:7, whole, :], field.at[at_group, 4:5, whole, :], (right, gy)),
            send(field.at[at_group, 7:8, whole, :], field.at[at_group, 5:6, whole, :], (left, gy)),
        ]
        halo += [send(cs3.at[k, at_pairs], cr3.at[k, at_pairs], corners[k]) for k in range(4)]
        halo += [
            send(field.at[at_group, 0:n, rows : rows + 8, :], field.at[at_group, 0:n, 0:8, :], (gx, up)),
            send(field.at[at_group, 0:n, 8:16, :], field.at[at_group, 0:n, 8 + rows : 16 + rows, :], (gx, down)),
        ]

        def finish():
            for copy in halo:
                copy.wait_recv()
            for t in range(g + 2):
                f, pair, half = (0, 2, 5)[g] + t, (0, 1, 3)[g] + t // 2, 4 * (t % 2)
                for k, (layer, row) in enumerate(((4, 4), (4, 8 + rows), (5, 4), (5, 8 + rows))):
                    field[f, layer, row : row + 4, :] = cr3[k, pair, half : half + 4, :]

        return finish

    def stresses(target, field, n, at):
        def layer(l):
            for k, (p, q) in enumerate(product_pairs):
                value = field[slots[3 + k], l, at, :] - field[slots[p], l, at, :] * field[slots[q], l, at, :]
                target[k, l] = value[:, : target.shape[3]]

        loop(n, layer)

    def level(g, field, n, rows, halo_of, wy, wz, put):
        half = n // 2

        def one_field(t):
            slot = (0, 2, 5)[g] + t
            index = 3 + lax.div((t + 1) * (6 - t), 2) + g - (6 - t)

            def along_x(i):
                at = pl.ds(pl.multiple_of(i * 8, 8), 8)
                p, q, next_even, next_odd = halo_of(slot, at)
                lift = Lift(lambda l: field[slot, l, at, :] if l < n else next_even)
                lift.known[("o1", -1)] = p + predict_one * lift.even(0)
                lift.known[("e1", -1)] = q + update_one * lift.odd_one(-1)
                lift.known[("o1", half)] = next_odd
                for k in range(half):
                    bands[k, at, :] = lift.low(k)
                    bands[half + k, at, :] = lift.high(k)

            loop(rows // 8 + 2, along_x)
            whole = rows + 16
            for k in range(0, n, 2):
                two = jnp.concatenate([bands[k, 0:whole, :], bands[k + 1, 0:whole, :]], axis=1)
                out = along_y(wy[k // half], two)
                mixed[k * rows : k * rows + rows, 0:128] = out[:, :128]
                mixed[k * rows + rows : k * rows + 2 * rows, 0:128] = out[:, 128:]
            out = along_z(mixed[0 : n * rows, 0:128], wz)
            for k in range(n):
                x_high, x_at = divmod(k, half)
                for y_high in range(2):
                    at = k * rows + y_high * (rows // 2)
                    for z_high in range(2):
                        value = out[at : at + rows // 2, 128 * z_high : 128 * z_high + 128]
                        put(index, slot, 4 * z_high + 2 * y_high + x_high, x_at, value)

        loop(g + 2, one_field)

    def halo_two(slot, at):
        return tuple(second[slot, 8 + l, at, :] for l in range(4))

    def put_two(index, slot, band, k, value):
        if band:
            d2[band - 1, index, k] = value[:, :64]
        else:
            third[slot, k, 8:24, :] = value

    def halo_three(slot, at):
        before, after = third[slot, 4, at, :], third[slot, 5, at, :]
        return before, pltpu.roll(before, 64, 1), after, pltpu.roll(after, 64, 1)

    def put_three(index, slot, band, k, value):
        if band:
            d3[band - 1, index, k] = value[:, :32]
        else:
            last[slot, k] = value

    for g in range(3):
        for copy in y_halo[g]:
            copy.wait_recv()
        loop(g + 2, lambda t: inner_field(g, t))
    for g in range(2):
        for copy in x_halo[g]:
            copy.wait_recv()
        if g == 0:
            unpack_corners(range(4))
        outer_group(g, "both")
        send_two(g, "right")
        send_two(g, "left")
    for side, which in (("right", 1), ("left", 0)):
        x_halo[2][which].wait_recv()
        outer_group(2, side)
        send_two(2, side)
    for g in range(3):
        outer_details(g, "both")
    stresses(s1, second, 8, slice(8, 40))
    finish_three = []
    for g in range(3):
        finish_two(g)
        level(g, second, 8, 32, halo_two, wy2, wz2, put_two)
        finish_three.append(exchange_three(g))
    stresses(s2, third, 4, slice(8, 24))
    for g in range(3):
        finish_three[g]()
        level(g, third, 4, 16, halo_three, wy3, wz3, put_three)
    stresses(s3, last, 2, slice(0, 8))
    for c in range(3):
        coarse[c] = last[slots[c]][:, :, :32]
    for copy in started:
        copy.wait_send()


def flush(*refs):
    sem = refs[14]
    copies = [pltpu.make_async_copy(refs[n].at[k], refs[7 + n].at[k], sem.at[n, k]) for n in (0, 2) for k in range(7)]
    copies += [pltpu.make_async_copy(refs[n], refs[7 + n], sem.at[n, 0]) for n in (1, 3, 4, 5, 6)]
    for copy in copies:
        copy.start()
    for copy in copies:
        copy.wait()


def body(velocity):
    shapes = ((7, 9, 8, 32, 128), (6, 8, 32, 128), (7, 9, 4, 16, 64), (6, 4, 16, 64), (7, 9, 2, 8, 32), (6, 2, 8, 32), (3, 2, 8, 32))
    copies = 16 + 24 + 24
    limit = 50_000_000
    run = pl.pallas_call(
        lambda *refs: kernel(lax.axis_size("gx"), lax.axis_size("gy"), *refs),
        out_shape=[pltpu.VMEM(shape, F32) for shape in shapes],
        in_specs=[pl.BlockSpec(memory_space=pltpu.HBM)] * 7,
        out_specs=[pl.BlockSpec(memory_space=pltpu.VMEM)] * 7,
        scratch_shapes=[
            pltpu.VMEM((4, 23, 80, 256), F32),
            pltpu.VMEM((9, 80, 256), F32),
            pltpu.VMEM((9, 7, 80, 256), F32),
            pltpu.VMEM((576, 256), F32),
            pltpu.VMEM((9, 16, 48, 128), F32),
            pltpu.VMEM((9, 8, 32, 128), F32),
            pltpu.VMEM((9, 2, 8, 128), F32),
            pltpu.VMEM((768, 256), BF16),
            pltpu.VMEM((384, 256), BF16),
            pltpu.VMEM((384, 256), BF16),
            pltpu.VMEM((2, 64, 256), BF16),
            pltpu.VMEM((2, 32, 144), BF16),
            pltpu.VMEM((2, 16, 96), BF16),
            pltpu.VMEM((4, 3, 2, 8, 256), F32),
            pltpu.VMEM((4, 3, 2, 8, 256), F32),
            pltpu.VMEM((4, 9, 8, 128), F32),
            pltpu.VMEM((4, 9, 8, 128), F32),
            pltpu.VMEM((4, 5, 8, 128), F32),
            pltpu.VMEM((4, 5, 8, 128), F32),
            pltpu.VMEM((8, 48, 128), F32),
            pltpu.SemaphoreType.DMA((9,)),
            pltpu.SemaphoreType.DMA((copies,)),
            pltpu.SemaphoreType.DMA((copies,)),
        ],
        compiler_params=pltpu.CompilerParams(collective_id=0, has_side_effects=True, vmem_limit_bytes=limit),
    )
    along_third = (third_table(256, 256), third_table(128, 128), third_table(64, 128))
    along_second = (second_table(64, 256), second_table(32, 144), second_table(16, 96))
    results = run(velocity, *along_third, *along_second)
    return tuple(
        pl.pallas_call(
            flush,
            out_shape=[pltpu.HBM(shape, F32) for shape in shapes],
            in_specs=[pl.BlockSpec(memory_space=pl.ANY)] * 7,
            out_specs=[pl.BlockSpec(memory_space=pl.ANY)] * 7,
            scratch_shapes=[pltpu.SemaphoreType.DMA((7, 7))],
            compiler_params=pltpu.CompilerParams(vmem_limit_bytes=1_000_000),
        )(*results)
    )


def solution(mesh):
    in_specs = (P(None, "gx", "gy", None),)
    out_specs = (
        P(None, None, "gx", "gy", None),
        P(None, "gx", "gy", None),
        P(None, None, "gx", "gy", None),
        P(None, "gx", "gy", None),
        P(None, None, "gx", "gy", None),
        P(None, "gx", "gy", None),
        P(None, "gx", "gy", None),
    )
    return jax.shard_map(body, mesh=mesh, in_specs=in_specs, out_specs=out_specs, check_vma=False)
```
